32 devices in a mesh: dp: 2 (over x), tp: 4 (over z), sq: 4 (over y, core).
Axes of the slice: x: 2, y: 2, z: 4, core: 2. Of those that a mesh axis runs over, the one named last changes fastest.
Arguments:
- x_steps: bfloat16 [4, 32, 6144], P(None, 'dp'), parts along dimension 1
- positions: int32 [32], P('dp'), parts along dimension 0
- k_cache: bfloat16 [32, 4096, 4, 128], P('dp', 'sq', 'tp'), parts along dimension 0
- v_cache: bfloat16 [32, 4096, 4, 128], P('dp', 'sq', 'tp'), parts along dimension 0
- w_q: bfloat16 [6144, 6144], P(None, 'tp')
- b_q: bfloat16 [6144], P('tp')
- w_k: bfloat16 [6144, 512], P(None, 'tp')
- b_k: bfloat16 [512], P('tp')
- w_v: bfloat16 [6144, 512], P(None, 'tp')
- b_v: bfloat16 [512], P('tp')
- w_o: bfloat16 [6144, 6144], P('tp')
- b_o: bfloat16 [6144], replicated
- ln1_gain: bfloat16 [6144], replicated
- ln1_bias: bfloat16 [6144], replicated
- ln2_gain: bfloat16 [6144], replicated
- ln2_bias: bfloat16 [6144], replicated
- w_fc: bfloat16 [6144, 24576], P(None, 'tp')
- b_fc: bfloat16 [24576], P('tp')
- w_proj: bfloat16 [24576, 6144], P('tp')
- b_proj: bfloat16 [6144], replicated
Outputs:
- output 1: bfloat16 [4, 32, 6144], P(None, 'dp'), parts along dimension 1
- output 2: bfloat16 [32, 4096, 4, 128], P('dp', 'sq', 'tp'), parts along dimension 0
- output 3: bfloat16 [32, 4096, 4, 128], P('dp', 'sq', 'tp'), parts along dimension 0
There are 2 independent parts. The reference program is written for one: setup_inputs(seed, part) draws one part's arguments, and reference() takes and returns one part's arrays. A program takes and returns all parts, laid end to end along the dimension named above; an argument that names none is the same for every part.
All inputs are finite; a program needn't handle non-finite values.
Results may differ from the reference program's by a relative error of at most 0.015911.
Values sent between devices are 32-bit elements.
A program may use at most 1 GiB of HBM per device.

```python
import jax
import jax.numpy as jnp
from jax import lax

D = 6144
HEADS = 48
KV_HEADS = 4
HEAD = 128
FF = 24576
WINDOW = 4096
BATCH = 16
STEPS = 4
ROPE_BASE = 1000000
POS_LOW = 100
POS_HIGH = 15000
HOT_ODDS = 512
HOT_RUN = 8


def rope_tables(positions, head_dim):
    half_dim = head_dim // 2
    inv_freq = jnp.power(jnp.float32(ROPE_BASE), -2.0 * jnp.arange(half_dim, dtype=jnp.float32) / head_dim)
    angle = positions.astype(jnp.float32)[..., None] * inv_freq
    return jnp.cos(angle), jnp.sin(angle)


def apply_rope(vectors, cos_t, sin_t):
    half_dim = vectors.shape[-1] // 2
    first = vectors[..., :half_dim]
    second = vectors[..., half_dim:]
    return jnp.concatenate([first * cos_t - second * sin_t, second * cos_t + first * sin_t], axis=-1)


def layer_norm(vectors, gain, shift):
    row_mean = jnp.mean(vectors, axis=-1, keepdims=True)
    centered = vectors - row_mean
    row_var = jnp.mean(centered * centered, axis=-1, keepdims=True)
    return centered * lax.rsqrt(row_var + 1e-5) * gain.astype(jnp.float32) + shift.astype(jnp.float32)


def linear(rows_in, weight, bias):
    return jnp.dot(rows_in, weight, preferred_element_type=jnp.float32) + bias.astype(jnp.float32)


def hot_direction():
    dim_ids = jnp.arange(HEAD)
    marked = (dim_ids % (HEAD // 2)) >= HEAD // 2 - 4
    return jnp.where(marked, 8.0 ** -0.5, 0.0).astype(jnp.float32)


def draw_positions(key):
    key_low, key_high, key_pick, key_perm = jax.random.split(key, 4)
    short = jax.random.randint(key_low, (BATCH,), POS_LOW, WINDOW)
    longer = jax.random.randint(key_high, (BATCH,), WINDOW, POS_HIGH + 1)
    chooser = jax.random.randint(key_pick, (BATCH,), 0, 4)
    mixed = jnp.where(chooser == 0, short, longer)
    mixed = mixed.at[0].set(POS_LOW).at[1].set(POS_HIGH)
    return jax.random.permutation(key_perm, mixed).astype(jnp.int32)


def setup_inputs(seed: int = 0, part: int = 0) -> dict:
    shared = jax.random.split(jax.random.key(seed), 16)
    own = jax.random.split(jax.random.fold_in(jax.random.key(seed + 1), part), 5)
    hot_amp = (8.0 * HEAD ** 0.5) ** 0.5
    hot_vec = hot_direction() * hot_amp
    positions = draw_positions(own[0])
    slot_ids = jnp.arange(WINDOW, dtype=jnp.int32)
    last_pos = positions[:, None] - 1
    held_pos = last_pos - (last_pos - slot_ids[None, :]) % WINDOW
    hot_slot = (jax.random.randint(own[1], (BATCH, WINDOW), 0, HOT_ODDS) == 0) | ((slot_ids[None, :] - positions[:, None]) % WINDOW < HOT_RUN)
    cos_t, sin_t = rope_tables(held_pos, HEAD)
    hot_keys = apply_rope(jnp.broadcast_to(hot_vec, (BATCH, WINDOW, HEAD)), cos_t, sin_t)
    hot_keys = jnp.where(hot_slot[:, :, None], hot_keys, 0.0)
    k_cache = (jax.random.normal(own[2], (BATCH, WINDOW, KV_HEADS, HEAD), jnp.float32) + hot_keys[:, :, None, :]).astype(jnp.bfloat16)
    v_cache = jax.random.normal(own[3], (BATCH, WINDOW, KV_HEADS, HEAD), jnp.float32).astype(jnp.bfloat16)
    x_steps = jax.random.normal(own[4], (STEPS, BATCH, D), jnp.float32).astype(jnp.bfloat16)

    def scaled(key, shape, scale):
        return (jax.random.normal(key, shape, jnp.float32) * scale).astype(jnp.bfloat16)

    b_q = (0.5 * jax.random.normal(shared[1], (HEADS * HEAD,), jnp.float32) + jnp.tile(hot_vec, HEADS)).astype(jnp.bfloat16)
    b_k = (0.5 * jax.random.normal(shared[3], (KV_HEADS * HEAD,), jnp.float32) + jnp.tile(hot_vec, KV_HEADS)).astype(jnp.bfloat16)
    return {
        "x_steps": x_steps,
        "positions": positions,
        "k_cache": k_cache,
        "v_cache": v_cache,
        "w_q": scaled(shared[0], (D, HEADS * HEAD), D ** -0.5),
        "b_q": b_q,
        "w_k": scaled(shared[2], (D, KV_HEADS * HEAD), D ** -0.5),
        "b_k": b_k,
        "w_v": scaled(shared[4], (D, KV_HEADS * HEAD), D ** -0.5),
        "b_v": scaled(shared[5], (KV_HEADS * HEAD,), 0.5),
        "w_o": scaled(shared[6], (HEADS * HEAD, D), 3.0 * (HEADS * HEAD) ** -0.5),
        "b_o": scaled(shared[7], (D,), 0.2),
        "ln1_gain": (1.0 + 0.2 * jax.random.normal(shared[8], (D,), jnp.float32)).astype(jnp.bfloat16),
        "ln1_bias": scaled(shared[9], (D,), 0.2),
        "ln2_gain": (1.0 + 0.2 * jax.random.normal(shared[10], (D,), jnp.float32)).astype(jnp.bfloat16),
        "ln2_bias": scaled(shared[11], (D,), 0.2),
        "w_fc": scaled(shared[12], (D, FF), D ** -0.5),
        "b_fc": scaled(shared[13], (FF,), 0.5),
        "w_proj": scaled(shared[14], (FF, D), 1.5 * FF ** -0.5),
        "b_proj": scaled(shared[15], (D,), 0.2),
    }


def reference(x_steps, positions, k_cache, v_cache, w_q, b_q, w_k, b_k, w_v, b_v, w_o, b_o,
              ln1_gain, ln1_bias, ln2_gain, ln2_bias, w_fc, b_fc, w_proj, b_proj):
    group = HEADS // KV_HEADS
    slot_ids = jnp.arange(WINDOW, dtype=jnp.int32)
    batch_ids = jnp.arange(BATCH, dtype=jnp.int32)
    score_scale = HEAD ** -0.5

    def attend_one(packed):
        q_one, k_one, v_one, slot_ok = packed
        scores = jnp.einsum("grd,wgd->grw", q_one.reshape(KV_HEADS, group, HEAD).astype(jnp.float32), k_one.astype(jnp.float32)) * score_scale
        scores = jnp.where(slot_ok[None, None, :], scores, -1e30)
        weights = jax.nn.softmax(scores, axis=-1)
        return jnp.einsum("grw,wgd->grd", weights, v_one.astype(jnp.float32))

    def one_step(carry, step_in):
        key_buf, val_buf = carry
        x_in, step_idx = step_in
        cur_pos = positions + step_idx
        hidden = layer_norm(x_in.astype(jnp.float32), ln1_gain, ln1_bias).astype(jnp.bfloat16)
        query = linear(hidden, w_q, b_q).astype(jnp.bfloat16)
        key_new = linear(hidden, w_k, b_k).astype(jnp.bfloat16)
        val_new = linear(hidden, w_v, b_v).astype(jnp.bfloat16)
        cos_t, sin_t = rope_tables(cur_pos, HEAD)
        q_rot = apply_rope(query.reshape(BATCH, HEADS, HEAD).astype(jnp.float32), cos_t[:, None, :], sin_t[:, None, :]).astype(jnp.bfloat16)
        k_rot = apply_rope(key_new.reshape(BATCH, KV_HEADS, HEAD).astype(jnp.float32), cos_t[:, None, :], sin_t[:, None, :]).astype(jnp.bfloat16)
        write_slot = cur_pos % WINDOW
        key_buf = key_buf.at[batch_ids, write_slot].set(k_rot)
        val_buf = val_buf.at[batch_ids, write_slot].set(val_new.reshape(BATCH, KV_HEADS, HEAD))
        held_pos = cur_pos[:, None] - (cur_pos[:, None] - slot_ids[None, :]) % WINDOW
        attn = lax.map(attend_one, (q_rot, key_buf, val_buf, held_pos >= 0))
        attn_out = attn.astype(jnp.bfloat16).reshape(BATCH, HEADS * HEAD)
        x_mid = (x_in.astype(jnp.float32) + jnp.dot(attn_out, w_o, preferred_element_type=jnp.float32) + b_o.astype(jnp.float32)).astype(jnp.bfloat16)
        hidden_two = layer_norm(x_mid.astype(jnp.float32), ln2_gain, ln2_bias).astype(jnp.bfloat16)
        gelu_out = jax.nn.gelu(linear(hidden_two, w_fc, b_fc), approximate=True).astype(jnp.bfloat16)
        y_out = (x_mid.astype(jnp.float32) + jnp.dot(gelu_out, w_proj, preferred_element_type=jnp.float32) + b_proj.astype(jnp.float32)).astype(jnp.bfloat16)
        return (key_buf, val_buf), y_out

    (k_final, v_final), y_steps = lax.scan(one_step, (k_cache, v_cache), (x_steps, jnp.arange(STEPS, dtype=jnp.int32)))
    return y_steps, k_final, v_final
```

```python
import functools

import jax
import jax.numpy as jnp
from jax import lax
from jax.experimental import pallas as pl
from jax.experimental.pallas import tpu as pltpu
from jax.sharding import PartitionSpec as P

ROPE_BASE = 1000000.0
LN_EPS = 1e-5
NEG_BIG = -1e30
MESH = pl.DeviceIdType.MESH

NCH = 6
CW = 512
NSUB = 6
NSLOT = 14


def layer_norm(vectors, gain, shift):
    row_mean = jnp.mean(vectors, axis=-1, keepdims=True)
    centered = vectors - row_mean
    row_var = jnp.mean(centered * centered, axis=-1, keepdims=True)
    return centered * lax.rsqrt(row_var + LN_EPS) * gain.astype(jnp.float32) + shift.astype(jnp.float32)


def rope_tables(positions, head_dim):
    half_dim = head_dim // 2
    inv_freq = jnp.power(jnp.float32(ROPE_BASE), -2.0 * jnp.arange(half_dim, dtype=jnp.float32) / head_dim)
    angle = positions.astype(jnp.float32)[..., None] * inv_freq
    return jnp.cos(angle), jnp.sin(angle)


def apply_rope(vectors, cos_t, sin_t):
    half_dim = vectors.shape[-1] // 2
    first = vectors[..., :half_dim]
    second = vectors[..., half_dim:]
    return jnp.concatenate([first * cos_t - second * sin_t, second * cos_t + first * sin_t], axis=-1)


def linear(rows_in, weight, bias):
    return jnp.dot(rows_in, weight, preferred_element_type=jnp.float32) + bias.astype(jnp.float32)


def tail_kernel(part, x_hbm, vecs, wo, wfc, wproj, out,
                rx, abuf, wobuf, wbuf, xbuf, mm1, dr1, cs1, cr1, x1buf, stat, hbuf, acc, gbuf,
                mm2, dr2, cs2, cr2, ybuf,
                wo_sem, w_sem, x_sem, rx_s, rx_r,
                d1_s, d1_r, c1_s, c1_r, st_s, st_r, h_cs, h_ds, h_r,
                d2_s, d2_r, c2_s, c2_r, y_cs, y_ds, y_ys, y_r):
    dp, z, sq = lax.axis_index("dp"), lax.axis_index("tp"), lax.axis_index("sq")
    y, c = sq // 2, sq % 2
    hw = NCH * CW
    pos = z + c * (3 - 2 * z)
    nxt = z + 1 - 2 * c
    prv = z - 1 + 2 * c
    f = z // 2
    own_first = c == f
    chip_core = (dp, z, 2 * y + 1 - c)
    chip_y = (dp, z, 2 * (1 - y) + c)
    chip_yc = (dp, z, 2 * (1 - y) + 1 - c)
    up = (dp, nxt, sq)
    down = (dp, prv, sq)
    stat_peer = (dp, 3 - z, 2 * y + 1 - c)

    def wo_copy(k):
        hs = jnp.where(k < NCH, f, 1 - f)
        j = k % NCH
        col = pl.multiple_of(hs * hw + j * CW, CW)
        return pltpu.make_async_copy(wo.at[pl.ds(pl.multiple_of(c * 768, 768), 768), pl.ds(col, CW)], wobuf.at[k], wo_sem.at[k])

    def fc_copy(k, i):
        hs = jnp.where(k < NCH, 1 - f, f)
        j = k % NCH
        row = pl.multiple_of(hs * hw + j * CW, CW)
        col = pl.multiple_of(c * hw + i * CW, CW)
        return pltpu.make_async_copy(wfc.at[pl.ds(row, CW), pl.ds(col, CW)], wbuf.at[k, i], w_sem.at[k, i])

    def pj_copy(k, i):
        slot = (k + 2 * NCH) % NSLOT
        hs = jnp.where(k < NCH, f, 1 - f)
        j = k % NCH
        row = pl.multiple_of(c * hw + i * CW, CW)
        col = pl.multiple_of(hs * hw + j * CW, CW)
        return pltpu.make_async_copy(wproj.at[pl.ds(row, CW), pl.ds(col, CW)], wbuf.at[slot, i], w_sem.at[slot, i])

    def x_copy():
        return pltpu.make_async_copy(x_hbm.at[pl.ds(2 * y, 2), :, pl.ds(pl.multiple_of(c * hw, hw), hw)], xbuf, x_sem)

    x_copy().start()

    @pl.loop(0, 2 * NCH)
    def _(k):
        wo_copy(k).start()

    @pl.loop(0, 2 * NCH)
    def _(k):
        for i in range(NSUB):
            fc_copy(k, i).start()

    @pl.loop(0, NSLOT - 2 * NCH)
    def _(k):
        for i in range(NSUB):
            pj_copy(k, i).start()

    bar = pltpu.get_barrier_semaphore()
    for dev in (chip_core, chip_y, chip_yc):
        pl.semaphore_signal(bar, inc=1, device_id=dev, device_id_type=MESH)

    @pl.when(pos < 3)
    def _():
        pl.semaphore_signal(bar, inc=1, device_id=up, device_id_type=MESH)

    @pl.when(pos > 0)
    def _():
        pl.semaphore_signal(bar, inc=1, device_id=down, device_id_type=MESH)

    @pl.when(pos == 3)
    def _():
        pl.semaphore_signal(bar, inc=1, device_id=stat_peer, device_id_type=MESH)
        pl.semaphore_wait(bar, 5)

    @pl.when(pos == 0)
    def _():
        pl.semaphore_wait(bar, 4)

    @pl.when((pos == 1) | (pos == 2))
    def _():
        pl.semaphore_wait(bar, 5)

    def remote(src, dst, ssem, rsem, dev):
        return pltpu.make_async_remote_copy(src_ref=src, dst_ref=dst, send_sem=ssem, recv_sem=rsem, device_id=dev, device_id_type=MESH)

    peers = (chip_y, chip_yc, chip_core)
    for n, dev in enumerate(peers):
        remote(part.at[dev[2]], rx.at[n], rx_s.at[n], rx_r.at[n], dev).start()
    for n, dev in enumerate(peers):
        remote(part.at[dev[2]], rx.at[n], rx_s.at[n], rx_r.at[n], dev).wait()
    stats = [part[sq, :, 768:896]] + [rx[n, :, 768:896] for n in range(3)]
    top = functools.reduce(jnp.maximum, stats)
    scale = [jnp.exp(s - top) for s in stats]
    for h in range(6):
        cols = slice(h * 128, (h + 1) * 128)
        outs = [part[sq, :, cols]] + [rx[n, :, cols] for n in range(3)]
        num = sum(o * r[:, h:h + 1] for o, r in zip(outs, scale))
        den = sum(s[:, 64 + h:65 + h] * r[:, h:h + 1] for s, r in zip(stats, scale))
        abuf[:, cols] = (num / den).astype(jnp.bfloat16)

    def reduce_chunks(product, mm, dr, cs, cr, d_s, d_r, c_s, c_r, finish):
        for phase in range(2):
            own = own_first if phase == 0 else jnp.logical_not(own_first)

            @pl.loop(0, NCH)
            def _(j):
                k = j + phase * NCH
                mm[k] = product(k)

                @pl.when(jnp.logical_not(own))
                def _():
                    remote(mm.at[k], dr.at[j], d_s.at[j], d_r.at[j], chip_core).start()

                @pl.when(own)
                def _():
                    remote(mm.at[k], dr.at[j], d_s.at[j], d_r.at[j], chip_core).wait_recv()
                    if phase == 0:
                        @pl.when(pos == 0)
                        def _():
                            cs[j] = mm[k] + dr[j]

                        @pl.when(pos == 1)
                        def _():
                            remote(cs.at[j], cr.at[j], c_s.at[j], c_r.at[j], up).wait_recv()
                            cs[j] = mm[k] + dr[j] + cr[j]

                        remote(cs.at[j], cr.at[j], c_s.at[j], c_r.at[j], up).start()
                    else:
                        remote(cs.at[j], cr.at[j], c_s.at[j], c_r.at[j], down).wait_recv()
                        total = mm[k] + dr[j] + cr[j]

                        @pl.when(pos == 2)
                        def _():
                            cs[j] = total
                            remote(cs.at[j], cr.at[j], c_s.at[j], c_r.at[j], up).start()

                        @pl.when(pos == 3)
                        def _():
                            finish(j, total)

    def vec(row, start):
        return vecs[pl.ds(row, 1), pl.ds(pl.multiple_of(start, CW), CW)]

    def wo_product(k):
        wo_copy(k).wait()
        return jnp.dot(abuf[...], wobuf[k], preferred_element_type=jnp.float32)

    def wo_finish(j, total):
        x_in = xbuf[:, :, pl.ds(pl.multiple_of(j * CW, CW), CW)].astype(jnp.float32).reshape(32, CW)
        x1buf[j] = (x_in + total + vec(0, c * hw + j * CW)).astype(jnp.bfloat16).astype(jnp.float32)

    x_copy().wait()
    reduce_chunks(wo_product, mm1, dr1, cs1, cr1, d1_s, d1_r, c1_s, c1_r, wo_finish)

    @pl.when(pos == 3)
    def _():
        mean = sum(jnp.sum(x1buf[j], axis=-1, keepdims=True) for j in range(NCH)) / hw
        m2 = 0.0
        for j in range(NCH):
            cen = x1buf[j] - mean
            m2 = m2 + jnp.sum(cen * cen, axis=-1, keepdims=True)
        lane = lax.broadcasted_iota(jnp.int32, (32, 128), 1)
        stat[0] = jnp.where(lane < 64, jnp.broadcast_to(mean, (32, 128)), jnp.broadcast_to(m2, (32, 128)))
        cp = remote(stat.at[0], stat.at[1], st_s, st_r, stat_peer)
        cp.start()
        cp.wait()
        mean_b, m2_b = stat[1, :, 0:1], stat[1, :, 64:65]
        diff = mean - mean_b
        row_mean = 0.5 * (mean + mean_b)
        row_var = (m2 + m2_b + diff * diff * (0.5 * hw)) / (2.0 * hw)
        inv = lax.rsqrt(row_var + LN_EPS)
        for j in range(NCH):
            hid = (x1buf[j] - row_mean) * inv * vec(1, c * hw + j * CW) + vec(2, c * hw + j * CW)
            hbuf[c, j] = hid.astype(jnp.bfloat16).astype(jnp.float32)
            remote(hbuf.at[c, j], hbuf.at[c, j], h_cs.at[j], h_r.at[c, j], down).start()
            remote(hbuf.at[c, j], hbuf.at[c, j], h_ds.at[j], h_r.at[c, j], chip_core).start()

    for i in range(NSUB):
        acc[:, i * CW:(i + 1) * CW] = jnp.broadcast_to(vec(4, c * hw + i * CW), (32, CW))

    def h_arrive(half, j):
        remote(hbuf.at[half, j], hbuf.at[half, j], h_cs.at[j], h_r.at[half, j], chip_core).wait_recv()

    def h_pass_down(j):
        remote(hbuf.at[c, j], hbuf.at[c, j], h_cs.at[j], h_r.at[c, j], down).start()

    def h_pass_core(j):
        remote(hbuf.at[c, j], hbuf.at[c, j], h_ds.at[j], h_r.at[c, j], chip_core).start()

    for phase in range(2):
        half = 1 - f if phase == 0 else f

        @pl.loop(0, NCH)
        def _(j):
            k = j + phase * NCH
            if phase == 0:
                @pl.when(own_first)
                def _():
                    h_arrive(1 - c, j)

                @pl.when(pos == 2)
                def _():
                    h_arrive(c, j)
                    h_pass_down(j)
                    h_pass_core(j)

                @pl.when((pos == 1) & (j >= 2))
                def _():
                    h_arrive(c, j - 2)
                    h_pass_down(j - 2)
                    h_pass_core(j - 2)
            else:
                @pl.when(jnp.logical_not(own_first))
                def _():
                    h_arrive(1 - c, j)

                @pl.when(pos == 0)
                def _():
                    h_arrive(c, j)
                    h_pass_core(j)

                @pl.when((pos == 1) & (j >= NCH - 2))
                def _():
                    h_arrive(c, j)
                    h_pass_down(j)
                    h_pass_core(j)

            for i in range(NSUB):
                fc_copy(k, i).wait()
            hid = hbuf[half, j].astype(jnp.bfloat16)
            for i in range(NSUB):
                cols = slice(i * CW, (i + 1) * CW)
                acc[:, cols] += jnp.dot(hid, wbuf[k, i], preferred_element_type=jnp.float32)

            @pl.when(k < 2 * NCH - (NSLOT - 2 * NCH))
            def _():
                for i in range(NSUB):
                    pj_copy(k + NSLOT - 2 * NCH, i).start()

    for i in range(NSUB):
        cols = slice(i * CW, (i + 1) * CW)
        gbuf[:, cols] = jax.nn.gelu(acc[:, cols], approximate=True).astype(jnp.bfloat16)

    def pj_product(k):
        slot = (k + 2 * NCH) % NSLOT
        for i in range(NSUB):
            pj_copy(k, i).wait()
        return sum(jnp.dot(gbuf[:, i * CW:(i + 1) * CW], wbuf[slot, i], preferred_element_type=jnp.float32) for i in range(NSUB))

    def y_pass_down(j):
        remote(ybuf.at[y, c, j], ybuf.at[y, c, j], y_cs.at[j], y_r.at[y, c, j], down).start()

    def y_pass_across(j):
        remote(ybuf.at[y, c, j], ybuf.at[y, c, j], y_ys.at[j], y_r.at[y, c, j], chip_y).start()

    def y_pass_core(side, j):
        remote(ybuf.at[side, c, j], ybuf.at[side, c, j], y_ds.at[side, j], y_r.at[side, c, j], chip_core).start()

    def y_arrive(side, half, j):
        remote(ybuf.at[side, half, j], ybuf.at[side, half, j], y_cs.at[j], y_r.at[side, half, j], chip_core).wait_recv()

    def pj_finish(j, total):
        ybuf[y, c, j] = (x1buf[j] + total + vec(3, c * hw + j * CW)).astype(jnp.bfloat16).astype(jnp.float32)
        y_pass_down(j)
        y_pass_across(j)
        y_pass_core(y, j)

    reduce_chunks(pj_product, mm2, dr2, cs2, cr2, d2_s, d2_r, c2_s, c2_r, pj_finish)

    def emit(side, half, j):
        col = pl.multiple_of(half * hw + j * CW, CW)
        out[pl.ds(2 * side, 2), :, pl.ds(col, CW)] = ybuf[side, half, j].reshape(2, 16, CW).astype(jnp.bfloat16)

    for j in range(NCH + 2):
        if j < NCH:
            @pl.when(pos < 3)
            def _():
                y_arrive(y, c, j)

                @pl.when(pos > 0)
                def _():
                    y_pass_down(j)

                y_pass_across(j)
                y_pass_core(y, j)

            emit(y, c, j)
        if j >= 2:
            y_arrive(1 - y, c, j - 2)
            y_pass_core(1 - y, j - 2)
            emit(1 - y, c, j - 2)

    @pl.loop(0, NCH)
    def _(j):
        y_arrive(y, 1 - c, j)
        emit(y, 1 - c, j)
        y_arrive(1 - y, 1 - c, j)
        emit(1 - y, 1 - c, j)

    @pl.loop(0, NCH)
    def _(j):
        remote(mm1.at[j], dr1.at[j], d1_s.at[j], d1_r.at[j], chip_core).wait_send()
        remote(mm2.at[j], dr2.at[j], d2_s.at[j], d2_r.at[j], chip_core).wait_send()
        remote(hbuf.at[c, j], hbuf.at[c, j], h_ds.at[j], h_r.at[c, j], chip_core).wait_send()
        remote(ybuf.at[y, c, j], ybuf.at[y, c, j], y_ys.at[j], y_r.at[y, c, j], chip_y).wait_send()
        for side in range(2):
            remote(ybuf.at[side, c, j], ybuf.at[side, c, j], y_ds.at[side, j], y_r.at[side, c, j], chip_core).wait_send()

        @pl.when(pos < 3)
        def _():
            remote(cs1.at[j], cr1.at[j], c1_s.at[j], c1_r.at[j], up).wait_send()
            remote(cs2.at[j], cr2.at[j], c2_s.at[j], c2_r.at[j], up).wait_send()

        @pl.when(pos > 0)
        def _():
            remote(hbuf.at[c, j], hbuf.at[c, j], h_cs.at[j], h_r.at[c, j], down).wait_send()
            remote(ybuf.at[y, c, j], ybuf.at[y, c, j], y_cs.at[j], y_r.at[y, c, j], down).wait_send()


def layer_tail(part, x_steps, vecs, w_o, w_fc, w_proj):
    hbm = pl.BlockSpec(memory_space=pltpu.HBM)
    vmem = pl.BlockSpec(memory_space=pltpu.VMEM)
    f32, bf16 = jnp.float32, jnp.bfloat16
    chunks = pltpu.VMEM((NCH, 32, CW), f32)
    dma = pltpu.SemaphoreType.DMA
    return pl.pallas_call(
        tail_kernel,
        out_shape=jax.ShapeDtypeStruct(x_steps.shape, bf16),
        in_specs=[vmem, hbm, vmem, hbm, hbm, hbm],
        out_specs=vmem,
        scratch_shapes=[
            pltpu.VMEM((3, 32, 896), f32), pltpu.VMEM((32, 768), bf16), pltpu.VMEM((2 * NCH, 768, CW), bf16),
            pltpu.VMEM((NSLOT, NSUB, CW, CW), bf16), pltpu.VMEM((2, 16, NCH * CW), bf16),
            pltpu.VMEM((2 * NCH, 32, CW), f32), chunks, chunks, chunks, chunks, pltpu.VMEM((2, 32, 128), f32),
            pltpu.VMEM((2, NCH, 32, CW), f32), pltpu.VMEM((32, NCH * CW), f32), pltpu.VMEM((32, NCH * CW), bf16),
            pltpu.VMEM((2 * NCH, 32, CW), f32), chunks, chunks, chunks, pltpu.VMEM((2, 2, NCH, 32, CW), f32),
            dma((2 * NCH,)), dma((NSLOT, NSUB)), dma, dma((3,)), dma((3,)),
            dma((NCH,)), dma((NCH,)), dma((NCH,)), dma((NCH,)), dma, dma, dma((NCH,)), dma((NCH,)), dma((2, NCH)),
            dma((NCH,)), dma((NCH,)), dma((NCH,)), dma((NCH,)), dma((NCH,)), dma((2, NCH)), dma((NCH,)), dma((2, 2, NCH)),
        ],
        compiler_params=pltpu.CompilerParams(collective_id=0, has_side_effects=True, vmem_limit_bytes=67043328),
    )(part, x_steps, vecs, w_o, w_fc, w_proj)


def attention_parts(x_steps, positions, k_cache, v_cache, w_q, b_q, w_k, b_k, w_v, b_v, ln1_gain, ln1_bias, sq_size):
    steps, batch, width = x_steps.shape
    slots_local, head_dim = k_cache.shape[1], k_cache.shape[3]
    heads = w_q.shape[1] // head_dim
    slots = slots_local * sq_size
    first_slot = lax.axis_index("sq") * slots_local
    slot_ids = first_slot + jnp.arange(slots_local, dtype=jnp.int32)
    step_ids = jnp.arange(steps, dtype=jnp.int32)
    hidden = layer_norm(x_steps.astype(jnp.float32), ln1_gain, ln1_bias).astype(jnp.bfloat16).reshape(steps * batch, width)
    query = linear(hidden, w_q, b_q).astype(jnp.bfloat16).reshape(steps, batch, heads, head_dim)
    key_new = linear(hidden, w_k, b_k).astype(jnp.bfloat16).reshape(steps, batch, head_dim)
    val_new = linear(hidden, w_v, b_v).astype(jnp.bfloat16).reshape(steps, batch, head_dim)
    cos_t, sin_t = rope_tables(positions[None, :] + step_ids[:, None], head_dim)
    q_rot = apply_rope(query.astype(jnp.float32), cos_t[:, :, None, :], sin_t[:, :, None, :]).astype(jnp.bfloat16)
    k_rot = apply_rope(key_new.astype(jnp.float32), cos_t, sin_t).astype(jnp.bfloat16)
    q_all = q_rot.transpose(1, 0, 2, 3).reshape(batch, steps * heads, head_dim)
    k_all, v_all = k_rot.transpose(1, 0, 2), val_new.transpose(1, 0, 2)
    age = (positions[:, None] - 1 - slot_ids[None, :]) % slots
    limit = jnp.minimum(positions[:, None] - 1, slots - 2 - step_ids[None, :])
    row_limit = jnp.repeat(limit, heads, axis=1)
    old_ok = age[:, None, :] <= row_limit[:, :, None]
    write_slot = (positions[:, None] + step_ids[None, :]) % slots - first_slot
    is_here = (write_slot >= 0) & (write_slot < slots_local)
    row_step = jnp.repeat(step_ids, heads)
    new_ok = is_here[:, None, :] & (step_ids[None, None, :] <= row_step[None, :, None])
    scale = head_dim ** -0.5
    k_old, v_old = k_cache[:, :, 0], v_cache[:, :, 0]
    s_old = jnp.where(old_ok, jnp.einsum("brd,bwd->brw", q_all, k_old, preferred_element_type=jnp.float32) * scale, NEG_BIG)
    s_new = jnp.where(new_ok, jnp.einsum("brd,bwd->brw", q_all, k_all, preferred_element_type=jnp.float32) * scale, NEG_BIG)
    top = jnp.maximum(jnp.max(s_old, axis=-1), jnp.max(s_new, axis=-1))
    w_old = jnp.where(old_ok, jnp.exp(s_old - top[..., None]), 0.0)
    w_new = jnp.where(new_ok, jnp.exp(s_new - top[..., None]), 0.0)
    total = jnp.sum(w_old, axis=-1) + jnp.sum(w_new, axis=-1)
    part = jnp.einsum("brw,bwd->brd", w_old.astype(jnp.bfloat16), v_old, preferred_element_type=jnp.float32)
    part = part + jnp.einsum("brw,bwd->brd", w_new.astype(jnp.bfloat16), v_all, preferred_element_type=jnp.float32)

    def arrange(t):
        n = t.shape[-1]
        return t.reshape(batch, 2, 2, 2, heads // 2, n).transpose(1, 3, 2, 0, 4, 5)

    outs = arrange(part).reshape(4, 32, 768)
    tops = arrange(top[..., None]).reshape(4, 32, 6)
    sums = arrange(total[..., None]).reshape(4, 32, 6)
    pad = ((0, 0), (0, 0), (0, 58))
    packed = jnp.concatenate([outs, jnp.pad(tops, pad), jnp.pad(sums, pad)], axis=-1)
    k_out, v_out = k_cache, v_cache
    target = jnp.where(is_here, write_slot, slots_local)
    batch_ids = jnp.arange(batch, dtype=jnp.int32)
    k_out = k_out.at[batch_ids[:, None], target].set(k_all[:, :, None, :], mode="drop")
    v_out = v_out.at[batch_ids[:, None], target].set(v_all[:, :, None, :], mode="drop")
    return packed, k_out, v_out


def solution(mesh):
    sq_size = mesh.shape["sq"]
    act_spec = P(None, "dp", None)
    cache_spec = P("dp", "sq", "tp", None)
    col_spec = P(None, "tp")
    row_spec = P("tp", None)
    vec_spec = P("tp")
    rep_spec = P(None)
    in_specs = (act_spec, P("dp"), cache_spec, cache_spec, col_spec, vec_spec, col_spec, vec_spec,
                col_spec, vec_spec, row_spec, rep_spec, rep_spec, rep_spec, rep_spec, rep_spec,
                col_spec, vec_spec, row_spec, rep_spec)
    out_specs = (act_spec, cache_spec, cache_spec)

    def per_device(x_steps, positions, k_cache, v_cache, w_q, b_q, w_k, b_k, w_v, b_v, w_o, b_o,
                   ln1_gain, ln1_bias, ln2_gain, ln2_bias, w_fc, b_fc, w_proj, b_proj):
        part, k_out, v_out = attention_parts(x_steps, positions, k_cache, v_cache, w_q, b_q, w_k, b_k, w_v, b_v,
                                             ln1_gain, ln1_bias, sq_size)
        vecs = jnp.stack([b_o, ln2_gain, ln2_bias, b_proj, b_fc, b_fc, b_fc, b_fc]).astype(jnp.float32)
        ys = layer_tail(part, x_steps, vecs, w_o, w_fc, w_proj)
        return ys, k_out, v_out

    return jax.shard_map(per_device, mesh=mesh, in_specs=in_specs, out_specs=out_specs, check_vma=False)
```
